32 devices in a mesh: gx: 4 (over z), gy: 2 (over x), gz: 4 (over y, core).
Axes of the slice: x: 2, y: 2, z: 4, core: 2. Of those that a mesh axis runs over, the one named last changes fastest.
Arguments:
- fields: bfloat16 [5, 128, 96, 512], P(None, 'gx', 'gy', 'gz'), may hold values from -8 to 8
Outputs:
- filtered: bfloat16 [5, 128, 96, 512], P(None, 'gx', 'gy', 'gz')
- stress: bfloat16 [15, 128, 96, 512], P(None, 'gx', 'gy', 'gz')
The draws below stay inside these ranges and needn't reach their ends.
All inputs are finite; a program needn't handle non-finite values.
Results may differ from the reference program's by a relative error of at most 0.0022.
Values may be sent and summed in bfloat16 or wider, within the bound.
A program may use at most 128 MiB of HBM per device.

```python
import jax
import jax.numpy as jnp
from jax import lax

R = 32
NX = 128
NY = 96
NZ = 512


def block_index(count):
    return (jnp.arange(count, dtype=jnp.int32) // 16).astype(jnp.int32)


def block_count(count):
    return (count + 15) // 16


def coarse_noise(key, shape):
    return jax.random.normal(key, shape, jnp.float32) * 0.9


def draw_fields(key, part):
    keys = jax.random.split(jax.random.fold_in(key, 17), 11)
    coord_x = (jnp.arange(NX, dtype=jnp.float32) + 0.5) / NX
    coord_y = jnp.arange(NY, dtype=jnp.float32) / NY
    coord_z = jnp.arange(NZ, dtype=jnp.float32) / NZ
    mixing = jax.random.normal(keys[0], (5, 5), jnp.float32) * 0.35 + jnp.eye(5, dtype=jnp.float32) * 0.8
    means = jax.random.uniform(keys[1], (5,), jnp.float32, -0.4, 0.4)
    jumps = jax.random.uniform(keys[2], (5,), jnp.float32, 0.2, 0.5)
    phases = jax.random.uniform(keys[3], (2,), jnp.float32, 0.0, 1.0)
    front = 0.5 + 0.12 * jnp.sin(2.0 * jnp.pi * (2.0 * coord_y[:, None] + phases[0])) + 0.08 * jnp.sin(2.0 * jnp.pi * (3.0 * coord_z[None, :] + phases[1]))
    distance = coord_x[:, None, None] - front[None, :, :]
    profile = jnp.tanh(distance / 0.08)
    envelope = 0.3 + 0.7 * jnp.exp(-(distance / 0.15) ** 2)
    line_x = jax.random.normal(keys[4], (5, NX + 1), jnp.float32)
    line_y = jax.random.normal(keys[5], (5, NY + 1), jnp.float32)
    line_z = jax.random.normal(keys[6], (5, NZ + 1), jnp.float32)
    bulk = jax.random.normal(keys[7], (5, NX, NY, NZ), jnp.float32)
    index_x = block_index(NX)
    index_y = block_index(NY)
    index_z = block_index(NZ)
    coarse_a = coarse_noise(keys[8], (5, NX, block_count(NY), block_count(NZ)))
    coarse_b = coarse_noise(keys[9], (5, block_count(NX), NY, block_count(NZ)))
    coarse_c = coarse_noise(keys[10], (5, block_count(NX), block_count(NY), NZ))
    white_x = jnp.take(jnp.take(coarse_a, index_y, axis=2), index_z, axis=3)
    white_y = jnp.take(jnp.take(coarse_b, index_x, axis=1), index_z, axis=3)
    white_z = jnp.take(jnp.take(coarse_c, index_x, axis=1), index_y, axis=2)
    step_x = (line_x[:, 1:] - line_x[:, :-1]) * 0.6
    step_y = (line_y[:, 1:] - line_y[:, :-1]) * 0.6
    step_z = (line_z[:, 1:] - line_z[:, :-1]) * 0.6
    rough = step_x[:, :, None, None] + step_y[:, None, :, None] + step_z[:, None, None, :] + 0.4 * envelope[None] * bulk + white_x + white_y + white_z
    mixed = jnp.einsum('cd,dxyz->cxyz', mixing, rough)
    values = means[:, None, None, None] + jumps[:, None, None, None] * profile[None] + mixed
    return jnp.clip(values, -8.0, 8.0).astype(jnp.bfloat16)


def setup_inputs(seed: int = 0) -> dict:
    splits = jax.random.split(jax.random.key(seed), 2)
    return {
        "fields": draw_fields(jax.random.fold_in(splits[1], 71), 0),
    }


pair_first = (0, 0, 0, 0, 0, 1, 1, 1, 1, 2, 2, 2, 3, 3, 4)
pair_second = (0, 1, 2, 3, 4, 1, 2, 3, 4, 2, 3, 4, 3, 4, 4)


def taps(offset):
    return jnp.where(jnp.abs(offset) <= R, 1.0, 0.0).astype(jnp.bfloat16)


def edge_norm(count, whole):
    cells = jnp.arange(count, dtype=jnp.int32)[:, None]
    offsets = jnp.arange(-R, R + 1, dtype=jnp.int32)[None, :]
    inside = (cells + offsets >= 0) & (cells + offsets < whole)
    return jnp.sum(jnp.where(inside, taps(offsets).astype(jnp.float32), 0.0), axis=1)


def reference(fields):
    offsets = jnp.arange(-R, R + 1, dtype=jnp.int32)
    weights = lax.optimization_barrier(taps(offsets)).astype(jnp.float32)
    total = jnp.sum(weights)
    norm_x = edge_norm(NX, NX)[:, None, None]

    def kernel(length):
        index = ((-offsets) % length).astype(jnp.int32)
        return jnp.zeros((length,), jnp.float32).at[index].add(weights)

    def along(values, axis, length):
        count = values.shape[axis]
        spectrum = jnp.fft.rfft(values, n=length, axis=axis)
        shape = [1, 1, 1]
        shape[axis] = -1
        factor = jnp.fft.rfft(kernel(length)).reshape(shape)
        result = jnp.fft.irfft(spectrum * factor, n=length, axis=axis)
        return lax.slice_in_dim(result, 0, count, axis=axis)

    def smooth_one(block):
        first = (along(block.astype(jnp.float32), 0, NX + 2 * R) / norm_x).astype(jnp.bfloat16)
        first = lax.optimization_barrier(first).astype(jnp.float32)
        second = (along(first, 2, NZ) / total).astype(jnp.bfloat16)
        second = lax.optimization_barrier(second).astype(jnp.float32)
        return along(second, 1, NY) / total

    smooth_fields = lax.map(smooth_one, fields)
    first_table = jnp.array(pair_first, jnp.int32)
    second_table = jnp.array(pair_second, jnp.int32)

    def pair_one(pair):
        left_index = first_table[pair]
        right_index = second_table[pair]
        left = lax.dynamic_index_in_dim(fields, left_index, 0, keepdims=False)
        right = lax.dynamic_index_in_dim(fields, right_index, 0, keepdims=False)
        product = (left.astype(jnp.float32) * right.astype(jnp.float32)).astype(jnp.bfloat16)
        smooth = smooth_one(product)
        mean_left = lax.dynamic_index_in_dim(smooth_fields, left_index, 0, keepdims=False)
        mean_right = lax.dynamic_index_in_dim(smooth_fields, right_index, 0, keepdims=False)
        return (smooth - mean_left * mean_right).astype(jnp.bfloat16)

    stress = lax.map(pair_one, jnp.arange(15, dtype=jnp.int32))
    return smooth_fields.astype(jnp.bfloat16), stress
```

```python
import functools

import jax
import jax.numpy as jnp
from jax import lax
from jax.experimental import pallas as pl
from jax.experimental.pallas import tpu as pltpu
from jax.sharding import PartitionSpec as P

R = 32


pair_first = (0, 0, 0, 0, 0, 1, 1, 1, 1, 2, 2, 2, 3, 3, 4)
pair_second = (0, 1, 2, 3, 4, 1, 2, 3, 4, 2, 3, 4, 3, 4, 4)


def padded(block, sides, width, periodic):
    for axis, dim in sides:
        count = lax.axis_size(axis)
        forward = [(i, i + 1) for i in range(count - 1)]
        if periodic:
            forward.append((count - 1, 0))
        backward = [(target, source) for source, target in forward]
        low = lax.ppermute(
            lax.slice_in_dim(block, block.shape[dim] - width, None, axis=dim), axis, forward
        )
        high = lax.ppermute(lax.slice_in_dim(block, 0, width, axis=dim), axis, backward)
        block = jnp.concatenate([low, block, high], axis=dim)
    return block


def taps(offset):
    return jnp.where(jnp.abs(offset) <= R, 1.0, 0.0).astype(jnp.bfloat16)


def banded(count):
    rows = lax.broadcasted_iota(jnp.int32, (count, count + 2 * R), 0)
    cols = lax.broadcasted_iota(jnp.int32, (count, count + 2 * R), 1)
    return taps(cols - rows - R)


def tap_total():
    offsets = jnp.arange(-R, R + 1, dtype=jnp.int32)
    return jnp.sum(taps(offsets).astype(jnp.float32))


def edge_norm(start, count, whole):
    cells = start + jnp.arange(count, dtype=jnp.int32)[:, None]
    offsets = jnp.arange(-R, R + 1, dtype=jnp.int32)[None, :]
    inside = (cells + offsets >= 0) & (cells + offsets < whole)
    return jnp.sum(jnp.where(inside, taps(offsets).astype(jnp.float32), 0.0), axis=1)


def streamwise_section(block, across, norm_x):
    plain = (
        jnp.einsum("im,cmyz->ciyz", across, block, preferred_element_type=jnp.float32) / norm_x
    ).astype(jnp.bfloat16)
    first_table = jnp.array(pair_first, jnp.int32)
    second_table = jnp.array(pair_second, jnp.int32)

    def product_filter(pair):
        left = lax.dynamic_index_in_dim(block, first_table[pair], 0, keepdims=False)
        right = lax.dynamic_index_in_dim(block, second_table[pair], 0, keepdims=False)
        product = (left.astype(jnp.float32) * right.astype(jnp.float32)).astype(jnp.bfloat16)
        result = jnp.einsum("im,myz->iyz", across, product, preferred_element_type=jnp.float32)
        return (result / norm_x).astype(jnp.bfloat16)

    products = lax.map(product_filter, jnp.arange(15, dtype=jnp.int32))
    return jnp.concatenate([plain, products], 0)


def finish(smooth):
    filtered = smooth[:5]
    stress = jnp.stack(
        [
            smooth[5 + pair] - smooth[pair_first[pair]] * smooth[pair_second[pair]]
            for pair in range(15)
        ],
        0,
    )
    return (filtered.astype(jnp.bfloat16), stress.astype(jnp.bfloat16))


def body(fields):
    depth_x = fields.shape[1]
    rimmed = padded(fields, (("gx", 1),), R, False)
    across = banded(depth_x)
    norm_x = edge_norm(lax.axis_index("gx") * depth_x, depth_x, depth_x * lax.axis_size("gx"))[
        :, None, None
    ]
    total = tap_total()
    widened = padded(rimmed, (("gz", 3),), R, True)
    zrimmed = streamwise_section(widened, across, norm_x)
    along_z = banded(fields.shape[3])
    zdone = (
        jnp.einsum("axyk,zk->axyz", zrimmed, along_z, preferred_element_type=jnp.float32) / total
    ).astype(jnp.bfloat16)
    yrimmed = padded(zdone, (("gy", 2),), R, True)
    along_y = banded(zdone.shape[2])
    smooth = (
        jnp.einsum("yj,axjz->axyz", along_y, yrimmed, preferred_element_type=jnp.float32) / total
    )
    filtered, stress = finish(smooth)
    return (filtered, stress)


def filter_kernel(dims, first_table, second_table, scale_x_ref, wz_ref, wy_ref, *refs):
    depth_x, half, depth_z = dims
    sources = refs[:20]
    filtered_ref, stress_ref, center, rims, narrow, means, sems = refs[20:]
    step = pl.program_id(0)
    rows = 2 * half
    inverse = 1.0 / (2 * R + 1)

    def copies(field):
        own, low, high, rim = sources[4 * field : 4 * field + 4]
        return [
            pltpu.make_async_copy(low, center.at[field, pl.ds(0, R)], sems.at[field, 0]),
            pltpu.make_async_copy(own, center.at[field, pl.ds(R, depth_x)], sems.at[field, 1]),
            pltpu.make_async_copy(high, center.at[field, pl.ds(R + depth_x, R)], sems.at[field, 2]),
            pltpu.make_async_copy(rim, rims.at[field], sems.at[field, 3]),
        ]

    @pl.when(step == 0)
    def _():
        for field in range(5):
            for copy in copies(field):
                copy.start()

    for field in range(5):

        @pl.when(step == field)
        def _(field=field):
            for copy in copies(field):
                copy.wait()

    left = first_table[step]
    right = second_table[step]

    def streamwise(source, count, column, plain):
        def chunk(index, carry):
            part = pl.ds(pl.multiple_of(index * 16, 16), 16)

            def value(row):
                one = source[left, row, part, :]
                if not plain:
                    one = one * source[right, row, part, :]
                return one.astype(jnp.float32)

            sums = [value(k) for k in range(4)]
            for row in range(4, 2 * R + 1):
                sums[row % 4] = sums[row % 4] + value(row)
            total = (sums[0] + sums[1]) + (sums[2] + sums[3])
            for cell in range(depth_x):
                if cell:
                    total = total + (value(cell + 2 * R) - value(cell - 1))
                narrow[cell, part, pl.ds(column, 128)] = (
                    total * scale_x_ref[cell]
                ).astype(jnp.bfloat16)
            return carry

        lax.fori_loop(0, count // 16, chunk, 0)

    def both(plain):
        streamwise(center, rows, 0, plain)
        streamwise(rims, half, depth_z, plain)

    pl.when(step < 5)(lambda: both(True))
    pl.when(step >= 5)(lambda: both(False))

    def smooth(cell):
        rim = narrow[cell, pl.ds(0, half), pl.ds(depth_z, 128)]
        parts = []
        for side in range(2):
            mid = narrow[cell, pl.ds(side * half, half), pl.ds(0, depth_z)]
            parts.append(
                jnp.dot(
                    jnp.concatenate([mid, rim], 1),
                    wz_ref[side],
                    preferred_element_type=jnp.float32,
                )
            )
        return (jnp.concatenate(parts, 0) * inverse).astype(jnp.bfloat16)

    def pairs(index, carry):
        for sub in range(2):
            cell = 4 * index + 2 * sub
            wide = jnp.concatenate([smooth(cell), smooth(cell + 1)], 1)
            out = jnp.dot(wy_ref[...], wide, preferred_element_type=jnp.float32) * inverse
            for k in range(2):
                g = out[:, k * depth_z : (k + 1) * depth_z]

                @pl.when(step < 5)
                def _(k=k, g=g):
                    means[step, cell + k] = g
                    filtered_ref[0, cell + k] = g.astype(jnp.bfloat16)

                @pl.when(step >= 5)
                def _(k=k, g=g):
                    stress_ref[0, cell + k] = (
                        g - means[left, cell + k] * means[right, cell + k]
                    ).astype(jnp.bfloat16)

        return carry

    lax.fori_loop(0, depth_x // 4, pairs, 0)


def shift(block, axis, by, periodic):
    count = lax.axis_size(axis)
    hops = [(i, (i + by) % count) for i in range(count) if periodic or 0 <= i + by < count]
    return lax.ppermute(block, axis, hops)


def compact(fields):
    _, depth_x, half, depth_z = fields.shape
    quarter = half // 2
    operands = []
    for field in range(5):
        mine = fields[field]
        own = jnp.concatenate([mine, shift(mine, "gy", 1, True)], 1)
        low = shift(own[depth_x - R :], "gx", 1, False)
        high = shift(own[:R], "gx", -1, False)

        def packed(columns):
            edge = jnp.concatenate([piece[:, :, columns] for piece in (low, own, high)], 0)
            return jnp.concatenate(
                [edge[:, k * quarter : (k + 1) * quarter] for k in range(4)], 2
            )

        def unpacked(block):
            quarters = [block[:, :, k * R : (k + 1) * R] for k in range(4)]
            return [
                jnp.concatenate(quarters[:2], 1),
                jnp.concatenate(quarters[2:], 1),
            ]

        before = shift(packed(slice(depth_z - R, depth_z)), "gz", 1, True)
        after = shift(packed(slice(0, R)), "gz", -1, True)
        rim = jnp.concatenate(unpacked(before) + unpacked(after), 2)
        operands += [own, low, high, rim]

    norm = edge_norm(lax.axis_index("gx") * depth_x, depth_x, depth_x * lax.axis_size("gx"))
    band = banded(depth_z).T
    blank = jnp.zeros((R, depth_z), jnp.bfloat16)
    lower, middle, upper = band[:R], band[R : R + depth_z], band[R + depth_z :]
    along_z = jnp.stack(
        [
            jnp.concatenate([middle, lower, blank, upper, blank], 0),
            jnp.concatenate([middle, blank, lower, blank, upper], 0),
        ]
    )
    rows = 2 * half
    gap = jnp.arange(rows)[None, :] - jnp.arange(half)[:, None]
    gap = (gap + half) % rows - half
    along_y = taps(gap)
    first_table = jnp.array(tuple(range(5)) + pair_first, jnp.int32)
    second_table = jnp.array(tuple(range(5)) + pair_second, jnp.int32)
    block = (1, depth_x, half, depth_z)
    smem = pl.BlockSpec(memory_space=pltpu.SMEM)
    vmem = pl.BlockSpec(memory_space=pltpu.VMEM)
    return pl.pallas_call(
        functools.partial(filter_kernel, (depth_x, half, depth_z)),
        grid=(20,),
        in_specs=[smem, smem, smem, vmem, vmem] + [pl.BlockSpec(memory_space=pl.ANY)] * 20,
        out_specs=[
            pl.BlockSpec(block, lambda c: (jnp.minimum(c, 4), 0, 0, 0)),
            pl.BlockSpec(block, lambda c: (jnp.maximum(c - 5, 0), 0, 0, 0)),
        ],
        out_shape=[
            jax.ShapeDtypeStruct((5,) + block[1:], jnp.bfloat16),
            jax.ShapeDtypeStruct((15,) + block[1:], jnp.bfloat16),
        ],
        scratch_shapes=[
            pltpu.VMEM((5, depth_x + 2 * R, rows, depth_z), jnp.bfloat16),
            pltpu.VMEM((5, depth_x + 2 * R, half, 4 * R), jnp.bfloat16),
            pltpu.VMEM((depth_x, rows, depth_z + 4 * R), jnp.bfloat16),
            pltpu.VMEM((5, depth_x, half, depth_z), jnp.float32),
            pltpu.SemaphoreType.DMA((5, 4)),
        ],
        compiler_params=pltpu.CompilerParams(vmem_limit_bytes=56 * 1024 * 1024),
    )(first_table, second_table, 1.0 / norm, along_z, along_y, *operands)


def solution(mesh):
    in_specs = (P(None, "gx", "gy", "gz"),)
    out_specs = (P(None, "gx", "gy", "gz"), P(None, "gx", "gy", "gz"))

    def local(fields):
        _, depth_x, half, depth_z = fields.shape
        fits = (
            mesh.shape["gy"] == 2
            and half % 16 == 0
            and 2 * half >= 2 * R + 1
            and depth_x >= R
            and depth_x % 4 == 0
            and depth_z == 4 * R
        )
        return tuple(compact(fields)) if fits else body(fields)

    return jax.shard_map(local, mesh=mesh, in_specs=in_specs, out_specs=out_specs, check_vma=False)
```

```python
import functools

import jax
import jax.numpy as jnp
from jax import lax
from jax.experimental import pallas as pl
from jax.experimental.pallas import tpu as pltpu
from jax.sharding import PartitionSpec as P

R = 32


pair_first = (0, 0, 0, 0, 0, 1, 1, 1, 1, 2, 2, 2, 3, 3, 4)
pair_second = (0, 1, 2, 3, 4, 1, 2, 3, 4, 2, 3, 4, 3, 4, 4)


def padded(block, sides, width, periodic):
    for axis, dim in sides:
        count = lax.axis_size(axis)
        forward = [(i, i + 1) for i in range(count - 1)]
        if periodic:
            forward.append((count - 1, 0))
        backward = [(target, source) for source, target in forward]
        low = lax.ppermute(
            lax.slice_in_dim(block, block.shape[dim] - width, None, axis=dim), axis, forward
        )
        high = lax.ppermute(lax.slice_in_dim(block, 0, width, axis=dim), axis, backward)
        block = jnp.concatenate([low, block, high], axis=dim)
    return block


def taps(offset):
    return jnp.where(jnp.abs(offset) <= R, 1.0, 0.0).astype(jnp.bfloat16)


def banded(count):
    rows = lax.broadcasted_iota(jnp.int32, (count, count + 2 * R), 0)
    cols = lax.broadcasted_iota(jnp.int32, (count, count + 2 * R), 1)
    return taps(cols - rows - R)


def tap_total():
    offsets = jnp.arange(-R, R + 1, dtype=jnp.int32)
    return jnp.sum(taps(offsets).astype(jnp.float32))


def edge_norm(start, count, whole):
    cells = start + jnp.arange(count, dtype=jnp.int32)[:, None]
    offsets = jnp.arange(-R, R + 1, dtype=jnp.int32)[None, :]
    inside = (cells + offsets >= 0) & (cells + offsets < whole)
    return jnp.sum(jnp.where(inside, taps(offsets).astype(jnp.float32), 0.0), axis=1)


def streamwise_section(block, across, norm_x):
    plain = (
        jnp.einsum("im,cmyz->ciyz", across, block, preferred_element_type=jnp.float32) / norm_x
    ).astype(jnp.bfloat16)
    first_table = jnp.array(pair_first, jnp.int32)
    second_table = jnp.array(pair_second, jnp.int32)

    def product_filter(pair):
        left = lax.dynamic_index_in_dim(block, first_table[pair], 0, keepdims=False)
        right = lax.dynamic_index_in_dim(block, second_table[pair], 0, keepdims=False)
        product = (left.astype(jnp.float32) * right.astype(jnp.float32)).astype(jnp.bfloat16)
        result = jnp.einsum("im,myz->iyz", across, product, preferred_element_type=jnp.float32)
        return (result / norm_x).astype(jnp.bfloat16)

    products = lax.map(product_filter, jnp.arange(15, dtype=jnp.int32))
    return jnp.concatenate([plain, products], 0)


def finish(smooth):
    filtered = smooth[:5]
    stress = jnp.stack(
        [
            smooth[5 + pair] - smooth[pair_first[pair]] * smooth[pair_second[pair]]
            for pair in range(15)
        ],
        0,
    )
    return (filtered.astype(jnp.bfloat16), stress.astype(jnp.bfloat16))


def body(fields):
    depth_x = fields.shape[1]
    rimmed = padded(fields, (("gx", 1),), R, False)
    across = banded(depth_x)
    norm_x = edge_norm(lax.axis_index("gx") * depth_x, depth_x, depth_x * lax.axis_size("gx"))[
        :, None, None
    ]
    total = tap_total()
    widened = padded(rimmed, (("gz", 3),), R, True)
    zrimmed = streamwise_section(widened, across, norm_x)
    along_z = banded(fields.shape[3])
    zdone = (
        jnp.einsum("axyk,zk->axyz", zrimmed, along_z, preferred_element_type=jnp.float32) / total
    ).astype(jnp.bfloat16)
    yrimmed = padded(zdone, (("gy", 2),), R, True)
    along_y = banded(zdone.shape[2])
    smooth = (
        jnp.einsum("yj,axjz->axyz", along_y, yrimmed, preferred_element_type=jnp.float32) / total
    )
    filtered, stress = finish(smooth)
    return (filtered, stress)


def filter_kernel(dims, first_table, second_table, scale_x_ref, wz_ref, wy_ref, *refs):
    depth_x, half, depth_z = dims
    sources = refs[:30]
    filtered_ref, stress_ref, center, rims, narrow, means, sems = refs[30:]
    step = pl.program_id(0)
    rows = 2 * half
    inverse = 1.0 / (2 * R + 1)

    def copies(field):
        parts = sources[6 * field : 6 * field + 6]
        places = ((R, depth_x), (0, R), (R + depth_x, R))
        return [
            pltpu.make_async_copy(
                parts[k], held.at[field, pl.ds(*places[k % 3])], sems.at[field, k]
            )
            for k, held in enumerate((center,) * 3 + (rims,) * 3)
        ]

    @pl.when(step == 0)
    def _():
        for field in range(5):
            for copy in copies(field):
                copy.start()

    for field in range(5):

        @pl.when(step == field)
        def _(field=field):
            for copy in copies(field):
                copy.wait()

    left = first_table[step]
    right = second_table[step]

    def streamwise(source, count, column, plain):
        def chunk(index, carry):
            part = pl.ds(pl.multiple_of(index * 16, 16), 16)

            def value(row):
                one = source[left, row, part, :]
                if not plain:
                    one = one * source[right, row, part, :]
                return one.astype(jnp.float32)

            sums = [value(k) for k in range(4)]
            for row in range(4, 2 * R + 1):
                sums[row % 4] = sums[row % 4] + value(row)
            total = (sums[0] + sums[1]) + (sums[2] + sums[3])
            for cell in range(depth_x):
                if cell:
                    total = total + (value(cell + 2 * R) - value(cell - 1))
                narrow[cell, part, pl.ds(column, 128)] = (
                    total * scale_x_ref[cell]
                ).astype(jnp.bfloat16)
            return carry

        lax.fori_loop(0, count // 16, chunk, 0)

    def both(plain):
        streamwise(center, rows, 0, plain)
        streamwise(rims, half, depth_z, plain)

    pl.when(step < 5)(lambda: both(True))
    pl.when(step >= 5)(lambda: both(False))

    def smooth(cell):
        rim = narrow[cell, pl.ds(0, half), pl.ds(depth_z, 128)]
        parts = []
        for side in range(2):
            mid = narrow[cell, pl.ds(side * half, half), pl.ds(0, depth_z)]
            parts.append(
                jnp.dot(
                    jnp.concatenate([mid, rim], 1),
                    wz_ref[side],
                    preferred_element_type=jnp.float32,
                )
            )
        return (jnp.concatenate(parts, 0) * inverse).astype(jnp.bfloat16)

    def pairs(index, carry):
        for sub in range(2):
            cell = 4 * index + 2 * sub
            wide = jnp.concatenate([smooth(cell), smooth(cell + 1)], 1)
            out = jnp.dot(wy_ref[...], wide, preferred_element_type=jnp.float32) * inverse
            for k in range(2):
                g = out[:, k * depth_z : (k + 1) * depth_z]

                @pl.when(step < 5)
                def _(k=k, g=g):
                    means[step, cell + k] = g
                    filtered_ref[0, cell + k] = g.astype(jnp.bfloat16)

                @pl.when(step >= 5)
                def _(k=k, g=g):
                    stress_ref[0, cell + k] = (
                        g - means[left, cell + k] * means[right, cell + k]
                    ).astype(jnp.bfloat16)

        return carry

    lax.fori_loop(0, depth_x // 4, pairs, 0)


def shift(block, axis, by, periodic):
    count = lax.axis_size(axis)
    hops = [(i, (i + by) % count) for i in range(count) if periodic or 0 <= i + by < count]
    return lax.ppermute(block, axis, hops)


def compact(fields):
    _, depth_x, half, depth_z = fields.shape
    quarter = half // 2
    operands = []
    for field in range(5):
        mine = fields[field]
        own = jnp.concatenate([mine, shift(mine, "gy", 1, True)], 1)
        low = shift(own[depth_x - R :], "gx", 1, False)
        high = shift(own[:R], "gx", -1, False)

        def packed(columns):
            edge = own[:, :, columns]
            return jnp.concatenate(
                [edge[:, k * quarter : (k + 1) * quarter] for k in range(4)], 2
            )

        def unpacked(block):
            quarters = [block[:, :, k * R : (k + 1) * R] for k in range(4)]
            return [
                jnp.concatenate(quarters[:2], 1),
                jnp.concatenate(quarters[2:], 1),
            ]

        before = shift(packed(slice(depth_z - R, depth_z)), "gz", 1, True)
        after = shift(packed(slice(0, R)), "gz", -1, True)
        rim = jnp.concatenate(unpacked(before) + unpacked(after), 2)
        rim_low = shift(rim[depth_x - R :], "gx", 1, False)
        rim_high = shift(rim[:R], "gx", -1, False)
        operands += [own, low, high, rim, rim_low, rim_high]

    norm = edge_norm(lax.axis_index("gx") * depth_x, depth_x, depth_x * lax.axis_size("gx"))
    band = banded(depth_z).T
    blank = jnp.zeros((R, depth_z), jnp.bfloat16)
    lower, middle, upper = band[:R], band[R : R + depth_z], band[R + depth_z :]
    along_z = jnp.stack(
        [
            jnp.concatenate([middle, lower, blank, upper, blank], 0),
            jnp.concatenate([middle, blank, lower, blank, upper], 0),
        ]
    )
    rows = 2 * half
    gap = jnp.arange(rows)[None, :] - jnp.arange(half)[:, None]
    gap = (gap + half) % rows - half
    along_y = taps(gap)
    first_table = jnp.array(tuple(range(5)) + pair_first, jnp.int32)
    second_table = jnp.array(tuple(range(5)) + pair_second, jnp.int32)
    block = (1, depth_x, half, depth_z)
    smem = pl.BlockSpec(memory_space=pltpu.SMEM)
    vmem = pl.BlockSpec(memory_space=pltpu.VMEM)
    return pl.pallas_call(
        functools.partial(filter_kernel, (depth_x, half, depth_z)),
        grid=(20,),
        in_specs=[smem, smem, smem, vmem, vmem] + [pl.BlockSpec(memory_space=pl.ANY)] * 30,
        out_specs=[
            pl.BlockSpec(block, lambda c: (jnp.minimum(c, 4), 0, 0, 0)),
            pl.BlockSpec(block, lambda c: (jnp.maximum(c - 5, 0), 0, 0, 0)),
        ],
        out_shape=[
            jax.ShapeDtypeStruct((5,) + block[1:], jnp.bfloat16),
            jax.ShapeDtypeStruct((15,) + block[1:], jnp.bfloat16),
        ],
        scratch_shapes=[
            pltpu.VMEM((5, depth_x + 2 * R, rows, depth_z), jnp.bfloat16),
            pltpu.VMEM((5, depth_x + 2 * R, half, 4 * R), jnp.bfloat16),
            pltpu.VMEM((depth_x, rows, depth_z + 4 * R), jnp.bfloat16),
            pltpu.VMEM((5, depth_x, half, depth_z), jnp.float32),
            pltpu.SemaphoreType.DMA((5, 6)),
        ],
        compiler_params=pltpu.CompilerParams(vmem_limit_bytes=56 * 1024 * 1024),
    )(first_table, second_table, 1.0 / norm, along_z, along_y, *operands)


def solution(mesh):
    in_specs = (P(None, "gx", "gy", "gz"),)
    out_specs = (P(None, "gx", "gy", "gz"), P(None, "gx", "gy", "gz"))

    def local(fields):
        _, depth_x, half, depth_z = fields.shape
        fits = (
            mesh.shape["gy"] == 2
            and half % 16 == 0
            and 2 * half >= 2 * R + 1
            and depth_x >= R
            and depth_x % 4 == 0
            and depth_z == 4 * R
        )
        return tuple(compact(fields)) if fits else body(fields)

    return jax.shard_map(local, mesh=mesh, in_specs=in_specs, out_specs=out_specs, check_vma=False)
```

```python
import functools

import jax
import jax.numpy as jnp
from jax import lax
from jax.experimental import pallas as pl
from jax.experimental.pallas import tpu as pltpu
from jax.sharding import PartitionSpec as P

R = 32


pair_first = (0, 0, 0, 0, 0, 1, 1, 1, 1, 2, 2, 2, 3, 3, 4)
pair_second = (0, 1, 2, 3, 4, 1, 2, 3, 4, 2, 3, 4, 3, 4, 4)


def padded(block, sides, width, periodic):
    for axis, dim in sides:
        count = lax.axis_size(axis)
        forward = [(i, i + 1) for i in range(count - 1)]
        if periodic:
            forward.append((count - 1, 0))
        backward = [(target, source) for source, target in forward]
        low = lax.ppermute(
            lax.slice_in_dim(block, block.shape[dim] - width, None, axis=dim), axis, forward
        )
        high = lax.ppermute(lax.slice_in_dim(block, 0, width, axis=dim), axis, backward)
        block = jnp.concatenate([low, block, high], axis=dim)
    return block


def taps(offset):
    return jnp.where(jnp.abs(offset) <= R, 1.0, 0.0).astype(jnp.bfloat16)


def banded(count):
    rows = lax.broadcasted_iota(jnp.int32, (count, count + 2 * R), 0)
    cols = lax.broadcasted_iota(jnp.int32, (count, count + 2 * R), 1)
    return taps(cols - rows - R)


def tap_total():
    offsets = jnp.arange(-R, R + 1, dtype=jnp.int32)
    return jnp.sum(taps(offsets).astype(jnp.float32))


def edge_norm(start, count, whole):
    cells = start + jnp.arange(count, dtype=jnp.int32)[:, None]
    offsets = jnp.arange(-R, R + 1, dtype=jnp.int32)[None, :]
    inside = (cells + offsets >= 0) & (cells + offsets < whole)
    return jnp.sum(jnp.where(inside, taps(offsets).astype(jnp.float32), 0.0), axis=1)


def streamwise_section(block, across, norm_x):
    plain = (
        jnp.einsum("im,cmyz->ciyz", across, block, preferred_element_type=jnp.float32) / norm_x
    ).astype(jnp.bfloat16)
    first_table = jnp.array(pair_first, jnp.int32)
    second_table = jnp.array(pair_second, jnp.int32)

    def product_filter(pair):
        left = lax.dynamic_index_in_dim(block, first_table[pair], 0, keepdims=False)
        right = lax.dynamic_index_in_dim(block, second_table[pair], 0, keepdims=False)
        product = (left.astype(jnp.float32) * right.astype(jnp.float32)).astype(jnp.bfloat16)
        result = jnp.einsum("im,myz->iyz", across, product, preferred_element_type=jnp.float32)
        return (result / norm_x).astype(jnp.bfloat16)

    products = lax.map(product_filter, jnp.arange(15, dtype=jnp.int32))
    return jnp.concatenate([plain, products], 0)


def finish(smooth):
    filtered = smooth[:5]
    stress = jnp.stack(
        [
            smooth[5 + pair] - smooth[pair_first[pair]] * smooth[pair_second[pair]]
            for pair in range(15)
        ],
        0,
    )
    return (filtered.astype(jnp.bfloat16), stress.astype(jnp.bfloat16))


def body(fields):
    depth_x = fields.shape[1]
    rimmed = padded(fields, (("gx", 1),), R, False)
    across = banded(depth_x)
    norm_x = edge_norm(lax.axis_index("gx") * depth_x, depth_x, depth_x * lax.axis_size("gx"))[
        :, None, None
    ]
    total = tap_total()
    widened = padded(rimmed, (("gz", 3),), R, True)
    zrimmed = streamwise_section(widened, across, norm_x)
    along_z = banded(fields.shape[3])
    zdone = (
        jnp.einsum("axyk,zk->axyz", zrimmed, along_z, preferred_element_type=jnp.float32) / total
    ).astype(jnp.bfloat16)
    yrimmed = padded(zdone, (("gy", 2),), R, True)
    along_y = banded(zdone.shape[2])
    smooth = (
        jnp.einsum("yj,axjz->axyz", along_y, yrimmed, preferred_element_type=jnp.float32) / total
    )
    filtered, stress = finish(smooth)
    return (filtered, stress)


def filter_kernel(dims, first_table, second_table, scale_x_ref, wz_ref, wy_ref, *refs):
    depth_x, half, depth_z = dims
    sources = refs[:30]
    filtered_ref, stress_ref, center, rims, narrow, means, sems = refs[30:]
    step = pl.program_id(0)
    rows = 2 * half
    inverse = 1.0 / (2 * R + 1)

    def copies(field):
        parts = sources[6 * field : 6 * field + 6]
        places = ((R, depth_x), (0, R), (R + depth_x, R))
        return [
            pltpu.make_async_copy(
                parts[k], held.at[field, pl.ds(*places[k % 3])], sems.at[field, k]
            )
            for k, held in enumerate((center,) * 3 + (rims,) * 3)
        ]

    @pl.when(step == 0)
    def _():
        for field in range(5):
            for copy in copies(field):
                copy.start()

    for field in range(5):

        @pl.when(step == field)
        def _(field=field):
            for copy in copies(field):
                copy.wait()

    left = first_table[step]
    right = second_table[step]

    def streamwise(source, count, column, plain):
        def chunk(index, carry):
            part = pl.ds(pl.multiple_of(index * 16, 16), 16)

            def value(row):
                one = source[left, row, part, :]
                if not plain:
                    one = one * source[right, row, part, :]
                return one.astype(jnp.float32)

            sums = [value(k) for k in range(4)]
            for row in range(4, 2 * R + 1):
                sums[row % 4] = sums[row % 4] + value(row)
            total = (sums[0] + sums[1]) + (sums[2] + sums[3])
            for cell in range(depth_x):
                if cell:
                    total = total + (value(cell + 2 * R) - value(cell - 1))
                narrow[cell, part, pl.ds(column, 128)] = (
                    total * scale_x_ref[cell]
                ).astype(jnp.bfloat16)
            return carry

        lax.fori_loop(0, count // 16, chunk, 0)

    def both(plain):
        streamwise(center, rows, 0, plain)
        streamwise(rims, half, depth_z, plain)

    pl.when(step < 5)(lambda: both(True))
    pl.when(step >= 5)(lambda: both(False))

    group = 8

    def spans(plain):
        def span(index, carry):
            cells = pl.ds(index * group, group)
            rim = narrow[cells, pl.ds(0, half), pl.ds(depth_z, 128)]
            rim = rim.reshape(group * half, 128)
            sides = []
            for side in range(2):
                mid = narrow[cells, pl.ds(side * half, half), pl.ds(0, depth_z)]
                smooth = jnp.dot(
                    jnp.concatenate([mid.reshape(group * half, depth_z), rim], 1),
                    wz_ref[side],
                    preferred_element_type=jnp.float32,
                )
                smooth = (smooth * inverse).astype(jnp.bfloat16)
                sides.append(smooth.reshape(group, half, depth_z))
            for pair in range(group // 2):
                wide = jnp.concatenate(
                    [
                        jnp.concatenate([part[2 * pair + k] for part in sides], 0)
                        for k in range(2)
                    ],
                    1,
                )
                out = jnp.dot(wy_ref[...], wide, preferred_element_type=jnp.float32) * inverse
                for k in range(2):
                    cell = index * group + 2 * pair + k
                    g = out[:, k * depth_z : (k + 1) * depth_z]
                    if plain:
                        means[step, cell] = g
                        filtered_ref[0, cell] = g.astype(jnp.bfloat16)
                    else:
                        stress_ref[0, cell] = (
                            g - means[left, cell] * means[right, cell]
                        ).astype(jnp.bfloat16)
            return carry

        lax.fori_loop(0, depth_x // group, span, 0)

    pl.when(step < 5)(lambda: spans(True))
    pl.when(step >= 5)(lambda: spans(False))


def shift(block, axis, by, periodic):
    count = lax.axis_size(axis)
    hops = [(i, (i + by) % count) for i in range(count) if periodic or 0 <= i + by < count]
    return lax.ppermute(block, axis, hops)


def compact(fields):
    _, depth_x, half, depth_z = fields.shape
    quarter = half // 2
    operands = []
    for field in range(5):
        mine = fields[field]
        own = jnp.concatenate([mine, shift(mine, "gy", 1, True)], 1)
        low = shift(own[depth_x - R :], "gx", 1, False)
        high = shift(own[:R], "gx", -1, False)

        def packed(columns):
            edge = own[:, :, columns]
            return jnp.concatenate(
                [edge[:, k * quarter : (k + 1) * quarter] for k in range(4)], 2
            )

        def unpacked(block):
            quarters = [block[:, :, k * R : (k + 1) * R] for k in range(4)]
            return [
                jnp.concatenate(quarters[:2], 1),
                jnp.concatenate(quarters[2:], 1),
            ]

        before = shift(packed(slice(depth_z - R, depth_z)), "gz", 1, True)
        after = shift(packed(slice(0, R)), "gz", -1, True)
        rim = jnp.concatenate(unpacked(before) + unpacked(after), 2)
        rim_low = shift(rim[depth_x - R :], "gx", 1, False)
        rim_high = shift(rim[:R], "gx", -1, False)
        operands += [own, low, high, rim, rim_low, rim_high]

    norm = edge_norm(lax.axis_index("gx") * depth_x, depth_x, depth_x * lax.axis_size("gx"))
    band = banded(depth_z).T
    blank = jnp.zeros((R, depth_z), jnp.bfloat16)
    lower, middle, upper = band[:R], band[R : R + depth_z], band[R + depth_z :]
    along_z = jnp.stack(
        [
            jnp.concatenate([middle, lower, blank, upper, blank], 0),
            jnp.concatenate([middle, blank, lower, blank, upper], 0),
        ]
    )
    rows = 2 * half
    gap = jnp.arange(rows)[None, :] - jnp.arange(half)[:, None]
    gap = (gap + half) % rows - half
    along_y = taps(gap)
    first_table = jnp.array(tuple(range(5)) + pair_first, jnp.int32)
    second_table = jnp.array(tuple(range(5)) + pair_second, jnp.int32)
    block = (1, depth_x, half, depth_z)
    smem = pl.BlockSpec(memory_space=pltpu.SMEM)
    vmem = pl.BlockSpec(memory_space=pltpu.VMEM)
    return pl.pallas_call(
        functools.partial(filter_kernel, (depth_x, half, depth_z)),
        grid=(20,),
        in_specs=[smem, smem, smem, vmem, vmem] + [pl.BlockSpec(memory_space=pl.ANY)] * 30,
        out_specs=[
            pl.BlockSpec(block, lambda c: (jnp.minimum(c, 4), 0, 0, 0)),
            pl.BlockSpec(block, lambda c: (jnp.maximum(c - 5, 0), 0, 0, 0)),
        ],
        out_shape=[
            jax.ShapeDtypeStruct((5,) + block[1:], jnp.bfloat16),
            jax.ShapeDtypeStruct((15,) + block[1:], jnp.bfloat16),
        ],
        scratch_shapes=[
            pltpu.VMEM((5, depth_x + 2 * R, rows, depth_z), jnp.bfloat16),
            pltpu.VMEM((5, depth_x + 2 * R, half, 4 * R), jnp.bfloat16),
            pltpu.VMEM((depth_x, rows, depth_z + 4 * R), jnp.bfloat16),
            pltpu.VMEM((5, depth_x, half, depth_z), jnp.float32),
            pltpu.SemaphoreType.DMA((5, 6)),
        ],
        compiler_params=pltpu.CompilerParams(vmem_limit_bytes=56 * 1024 * 1024),
    )(first_table, second_table, 1.0 / norm, along_z, along_y, *operands)


def solution(mesh):
    in_specs = (P(None, "gx", "gy", "gz"),)
    out_specs = (P(None, "gx", "gy", "gz"), P(None, "gx", "gy", "gz"))

    def local(fields):
        _, depth_x, half, depth_z = fields.shape
        fits = (
            mesh.shape["gy"] == 2
            and half % 16 == 0
            and 2 * half >= 2 * R + 1
            and depth_x >= R
            and depth_x % 8 == 0
            and depth_z == 4 * R
        )
        return tuple(compact(fields)) if fits else body(fields)

    return jax.shard_map(local, mesh=mesh, in_specs=in_specs, out_specs=out_specs, check_vma=False)
```
